32 devices in a mesh: dp: 16 (over z, x, core), tensor: 2 (over y).
Axes of the slice: x: 2, y: 2, z: 4, core: 2. Of those that a mesh axis runs over, the one named last changes fastest.
Arguments:
- tokens: float32 [8192, 2048], P(('dp', 'tensor')), may hold values from -6 to 6
- cotangent: float32 [8192, 2048], P(('dp', 'tensor')), may hold values from -6 to 6
- lengths: int32 [16, 4], P('dp'), may hold values from 32 to 224, as said below
- qkv_master: float32 [2048, 6144], P('dp', 'tensor'), may hold values from -0.125 to 0.125
- qkv_first: float32 [2048, 6144], P('dp', 'tensor'), may hold values from -32 to 32
- qkv_second: float32 [2048, 6144], P('dp', 'tensor'), may hold values from 106.496 to 434.176
- qkv_average: float32 [2048, 6144], P('dp', 'tensor'), may hold values from -0.125 to 0.125
- out_master: float32 [2048, 2048], P('tensor', 'dp'), may hold values from -1 to 1
- out_first: float32 [2048, 2048], P('tensor', 'dp'), may hold values from -10 to 10
- out_second: float32 [2048, 2048], P('tensor', 'dp'), may hold values from 9.8304 to 38.5024
- out_average: float32 [2048, 2048], P('tensor', 'dp'), may hold values from -1 to 1
- up_master: float32 [2048, 8192], P('dp', 'tensor'), may hold values from -0.125 to 0.125
- up_first: float32 [2048, 8192], P('dp', 'tensor'), may hold values from -20 to 20
- up_second: float32 [2048, 8192], P('dp', 'tensor'), may hold values from 52.4288 to 212.992
- up_average: float32 [2048, 8192], P('dp', 'tensor'), may hold values from -0.125 to 0.125
- down_master: float32 [8192, 2048], P('tensor', 'dp'), may hold values from -0.0625 to 0.0625
- down_first: float32 [8192, 2048], P('tensor', 'dp'), may hold values from -32 to 32
- down_second: float32 [8192, 2048], P('tensor', 'dp'), may hold values from 155.648 to 622.592
- down_average: float32 [8192, 2048], P('tensor', 'dp'), may hold values from -0.0625 to 0.0625
- norm_master: float32 [4, 2048], replicated, as said below
- norm_first: float32 [4, 2048], replicated, may hold values from -56 to 56
- norm_second: float32 [4, 2048], replicated, may hold values from 409.6 to 1638.4
- norm_average: float32 [4, 2048], replicated, as said below
Outputs:
- layer_out: float32 [8192, 2048], P(('dp', 'tensor'))
- input_grad: float32 [8192, 2048], P(('dp', 'tensor'))
- qkv_master_new: float32 [2048, 6144], P('dp', 'tensor')
- qkv_first_new: float32 [2048, 6144], P('dp', 'tensor')
- qkv_second_new: float32 [2048, 6144], P('dp', 'tensor')
- qkv_copy_new: bfloat16 [2048, 6144], P('dp', 'tensor')
- qkv_average_new: float32 [2048, 6144], P('dp', 'tensor')
- out_master_new: float32 [2048, 2048], P('tensor', 'dp')
- out_first_new: float32 [2048, 2048], P('tensor', 'dp')
- out_second_new: float32 [2048, 2048], P('tensor', 'dp')
- out_copy_new: bfloat16 [2048, 2048], P('tensor', 'dp')
- out_average_new: float32 [2048, 2048], P('tensor', 'dp')
- up_master_new: float32 [2048, 8192], P('dp', 'tensor')
- up_first_new: float32 [2048, 8192], P('dp', 'tensor')
- up_second_new: float32 [2048, 8192], P('dp', 'tensor')
- up_copy_new: bfloat16 [2048, 8192], P('dp', 'tensor')
- up_average_new: float32 [2048, 8192], P('dp', 'tensor')
- down_master_new: float32 [8192, 2048], P('tensor', 'dp')
- down_first_new: float32 [8192, 2048], P('tensor', 'dp')
- down_second_new: float32 [8192, 2048], P('tensor', 'dp')
- down_copy_new: bfloat16 [8192, 2048], P('tensor', 'dp')
- down_average_new: float32 [8192, 2048], P('tensor', 'dp')
- norm_master_new: float32 [4, 2048], replicated
- norm_first_new: float32 [4, 2048], replicated
- norm_second_new: float32 [4, 2048], replicated
- norm_copy_new: bfloat16 [4, 2048], replicated
- norm_average_new: float32 [4, 2048], replicated
The draws below stay inside these ranges and needn't reach their ends.
Inputs may be any that keep to these rules, and one draw needn't show every extreme that they name: Row g holds the lengths of the 4 sequences of group g in order; each consecutive pair fills exactly the 256 rows of one device, so no sequence crosses a device's rows; some sequence has exactly 224 tokens. `norm_master`: rows 0 and 2 are gains, rows 1 and 3 shifts. `norm_average`: rows 0 and 2 are gains, rows 1 and 3 shifts.
All inputs are finite; a program needn't handle non-finite values.
Results may differ from the reference program's by a relative error of at most 0.0038.
The reference program's roundings to bfloat16 on the way count: a program that leaves them out, or rounds other values in their place, can miss the bound.
Values may be sent and summed in bfloat16 or wider, within the bound.
A program may use at most 320 MiB of HBM per device.

```python
import math
import jax
import jax.numpy as jnp
from jax import lax

D = 2048
HEADS = 8
HS = 256
ROT = 64
FF = 8192
TOK_DEV = 256
STEP = 7
SEQS = 4
GROUP = 512
TOKENS = 8192
MAXLEN = 224
N_DP = 16
N_TENSOR = 2


def norm_table(key, salt_value):
    folded = jax.random.fold_in(key, salt_value)
    gain_key, shift_key = jax.random.split(folded)
    gain_rows = jax.random.uniform(gain_key, (2, D), jnp.float32, 0.6, 1.4)
    shift_rows = 0.4 * jax.random.normal(shift_key, (2, D), jnp.float32)
    return jnp.stack([gain_rows[0], shift_rows[0], gain_rows[1], shift_rows[1]], axis=0)


def draw_norm_master(key, part):
    return norm_table(key, 11)


def draw_norm_average(key, part):
    return norm_table(key, 23)


def draw_lengths(key, part):
    folded = jax.random.fold_in(key, 37)
    first = jax.random.randint(folded, (N_DP, N_TENSOR), TOK_DEV // 8, MAXLEN + 1, dtype=jnp.int32)
    first = first.at[0, 0].set(MAXLEN)
    second = (TOK_DEV - first).astype(jnp.int32)
    return jnp.stack([first, second], axis=-1).reshape(N_DP, SEQS).astype(jnp.int32)


def raised(values, rng, source, target, parts, factor):
    owner, partner = [(jnp.arange(values.shape[dim]) // (values.shape[dim] // parts)).reshape([-1 if axis == dim else 1 for axis in range(values.ndim)]) for dim in (source, target)]
    chosen = jax.random.permutation(rng, parts)[partner]
    strong = (owner == chosen) | (owner == (partner + parts // 2) % parts)
    return jnp.where(strong, factor * values, values)


def levels(key, extent, cuts, low, largest):
    level, own = 1.0, jax.random.fold_in(key, 6)
    for axis_at, blocks in cuts:
        heights = jnp.exp(jax.random.uniform(jax.random.fold_in(own, axis_at), (blocks,), jnp.float32, low / len(cuts), largest / len(cuts)))
        level = level * jnp.repeat(heights, extent[axis_at] // blocks).reshape([-1 if axis == axis_at else 1 for axis in range(len(extent))])
    return level


def scatter_about(key, extent, deviation, limit, shards=(), held_as=jnp.bfloat16):
    values = jax.random.normal(key, extent, jnp.float32) * deviation
    if len(shards) > 0:
        values = levels(key, extent, shards, -0.22, 0.18) * values
    return jnp.clip(values, min=-limit, max=limit).astype(held_as)


def heavy_noise(key, extent, deviation, bound, cuts, heavy, kind=jnp.bfloat16):
    values = deviation * jax.random.normal(key, extent, jnp.float32)
    if cuts:
        values = values * levels(key, extent, cuts, -0.22, 0.18)
    return jnp.clip(raised(values, jax.random.fold_in(key, 3), *heavy), -bound, bound).astype(kind)


def setup_inputs(seed: int = 0) -> dict:
    keys = jax.random.split(jax.random.key(seed), 24)
    tokens = scatter_about(keys[0], (TOKENS, D), 1.0, 6.0, ((0, 32),), jnp.float32)
    cotangent = heavy_noise(keys[1], (TOKENS, D), 1.0, 6.0, ((0, 32),), (0, 1, 32, 2.75), jnp.float32)
    lengths = draw_lengths(jax.random.fold_in(keys[23], 71), 0)
    qkv_master = scatter_about(keys[3], (D, 3 * D), D ** -0.5, 0.125, ((0, 16), (1, 2)), jnp.float32)
    qkv_first = scatter_about(keys[4], (D, 3 * D), (0.055 * TOKENS ** 0.5), 32.0, ((0, 16), (1, 2)), jnp.float32)
    qkv_second = jnp.clip(jnp.exp(math.log(434.176) - 1.40534252 * jax.random.uniform(keys[5], (D, 3 * D), jnp.float32) ** levels(keys[5], (D, 3 * D), ((0, 16), (1, 2)), -0.2, 0.2)), 106.496, 434.176)
    qkv_average = scatter_about(keys[6], (D, 3 * D), D ** -0.5, 0.125, ((0, 16), (1, 2)), jnp.float32)
    out_master = scatter_about(keys[7], (D, D), (D // 64) ** -0.5, 1.0, ((0, 2), (1, 16)), jnp.float32)
    out_first = scatter_about(keys[8], (D, D), (0.017 * TOKENS ** 0.5), 10.0, ((0, 2), (1, 16)), jnp.float32)
    out_second = jnp.clip(jnp.exp(math.log(38.5024) - 1.3652409 * jax.random.uniform(keys[9], (D, D), jnp.float32) ** levels(keys[9], (D, D), ((0, 2), (1, 16)), -0.2, 0.2)), 9.8304, 38.5024)
    out_average = scatter_about(keys[10], (D, D), (D // 64) ** -0.5, 1.0, ((0, 2), (1, 16)), jnp.float32)
    up_master = scatter_about(keys[11], (D, FF), D ** -0.5, 0.125, ((0, 16), (1, 2)), jnp.float32)
    up_first = scatter_about(keys[12], (D, FF), (0.039 * TOKENS ** 0.5), 20.0, ((0, 16), (1, 2)), jnp.float32)
    up_second = jnp.clip(jnp.exp(math.log(212.992) - 1.4017986 * jax.random.uniform(keys[13], (D, FF), jnp.float32) ** levels(keys[13], (D, FF), ((0, 16), (1, 2)), -0.2, 0.2)), 52.4288, 212.992)
    up_average = scatter_about(keys[14], (D, FF), D ** -0.5, 0.125, ((0, 16), (1, 2)), jnp.float32)
    down_master = scatter_about(keys[15], (FF, D), FF ** -0.5, 0.0625, ((0, 2), (1, 16)), jnp.float32)
    down_first = scatter_about(keys[16], (FF, D), (0.067 * TOKENS ** 0.5), 32.0, ((0, 2), (1, 16)), jnp.float32)
    down_second = jnp.clip(jnp.exp(math.log(622.592) - 1.3862944 * jax.random.uniform(keys[17], (FF, D), jnp.float32) ** levels(keys[17], (FF, D), ((0, 2), (1, 16)), -0.2, 0.2)), 155.648, 622.592)
    down_average = scatter_about(keys[18], (FF, D), FF ** -0.5, 0.0625, ((0, 2), (1, 16)), jnp.float32)
    norm_master = draw_norm_master(jax.random.fold_in(keys[23], 71), 0)
    norm_first = scatter_about(keys[20], (4, D), (0.1 * TOKENS ** 0.5), 56.0, (), jnp.float32)
    norm_second = jnp.clip(jnp.exp(jax.random.uniform(keys[21], (4, D), jnp.float32, math.log(409.6), math.log(1638.4))), 409.6, 1638.4)
    norm_average = draw_norm_average(jax.random.fold_in(keys[23], 71), 0)
    return dict(tokens=tokens, cotangent=cotangent, lengths=lengths, qkv_master=qkv_master, qkv_first=qkv_first, qkv_second=qkv_second, qkv_average=qkv_average, out_master=out_master, out_first=out_first, out_second=out_second, out_average=out_average, up_master=up_master, up_first=up_first, up_second=up_second, up_average=up_average, down_master=down_master, down_first=down_first, down_second=down_second, down_average=down_average, norm_master=norm_master, norm_first=norm_first, norm_second=norm_second, norm_average=norm_average)


@jax.custom_vjp
def low(v):
    return lax.optimization_barrier(v.astype(jnp.bfloat16)).astype(jnp.float32)

@jax.custom_vjp
def low_back(v):
    return v

def low_keep(v):
    return (low(v), None)

def low_pass(kept, grad):
    return (grad,)

def back_keep(v):
    return (v, None)

def back_low(kept, grad):
    return (low(grad),)
low.defvjp(low_keep, low_pass)
low_back.defvjp(back_keep, back_low)
highest = lax.Precision.HIGHEST
beta_one = 0.9
beta_two = 0.95
epsilon = 1e-08
average_rate = 0.9

def layer_norm(rows_in, gain_row, shift_row):
    average = lax.optimization_barrier(jnp.mean(rows_in, axis=-1, keepdims=True))
    centered = rows_in - average
    variance = lax.optimization_barrier(jnp.mean(centered * centered, axis=-1, keepdims=True))
    return centered * lax.rsqrt(variance + 1e-05) * gain_row + shift_row

def layout(length_row):
    seq_ends = jnp.cumsum(length_row).astype(jnp.int32)
    seq_starts = (seq_ends - length_row).astype(jnp.int32)
    row_index = jnp.arange(GROUP, dtype=jnp.int32)
    segment = lax.optimization_barrier(jnp.sum((row_index[:, None] >= seq_ends[None, :]).astype(jnp.int32), axis=1))
    onehot = segment[:, None] == jnp.arange(SEQS, dtype=jnp.int32)[None, :]
    row_start = lax.optimization_barrier(jnp.sum(jnp.where(onehot, seq_starts[None, :], 0), axis=1)).astype(jnp.int32)
    return (segment, row_index, (row_index - row_start).astype(jnp.float32))

def rotary_tables(position):
    half_rot = ROT // 2
    exponent = jnp.arange(half_rot, dtype=jnp.float32) * (2.0 / ROT)
    inverse = jnp.exp(-math.log(10000.0) * exponent)
    angles = position[:, None] * inverse[None, :]
    return (jnp.cos(angles), jnp.sin(angles))

def rotate(vectors, cosine, sine_table):
    half_rot = ROT // 2
    first_part = vectors[..., :half_rot]
    second_part = vectors[..., half_rot:ROT]
    rest_part = vectors[..., ROT:]
    cos_b = cosine[:, None, :]
    sin_b = sine_table[:, None, :]
    return jnp.concatenate([first_part * cos_b - second_part * sin_b, second_part * cos_b + first_part * sin_b, rest_part], axis=-1)

def group_forward(lowered, norms, rows_in, length_row):
    w_qkv, w_out, w_up, w_down = lowered
    segment, row_index, position = layout(length_row)
    normed_one = low(layer_norm(rows_in, norms[0], norms[1]))
    normed_two = low(layer_norm(rows_in, norms[2], norms[3]))
    joined_qkv = low_back(jnp.dot(normed_one, w_qkv, precision=highest)).reshape(GROUP, HEADS, 3, HS)
    cosine, sine_table = rotary_tables(position)
    query_low = low(rotate(joined_qkv[:, :, 0], cosine, sine_table))
    key_low = low(rotate(joined_qkv[:, :, 1], cosine, sine_table))
    value_low = low(joined_qkv[:, :, 2])
    scores = low_back(jnp.einsum('qhd,khd->hqk', query_low, key_low, precision=highest) * HS ** (-0.5))
    allowed = (segment[:, None] == segment[None, :]) & (row_index[:, None] >= row_index[None, :])
    scores = jnp.where(allowed[None], scores, -1e+30)
    probs_low = low(jax.nn.softmax(scores, axis=-1))
    mixed_heads = low(low_back(jnp.einsum('hqk,khd->qhd', probs_low, value_low, precision=highest))).reshape(GROUP, D)
    attended = jnp.dot(mixed_heads, w_out, precision=highest)
    upward = low_back(jnp.dot(normed_two, w_up, precision=highest))
    active = low(jax.nn.gelu(upward, approximate=False))
    branch = low_back(attended + jnp.dot(active, w_down, precision=highest))
    return rows_in + branch

def forward(rows_in, w_qkv, w_out, w_up, w_down, norms, lengths):
    lowered = (low(w_qkv), low(w_out), low(w_up), low(w_down))
    grouped = rows_in.reshape(N_DP, GROUP, D)
    step_fn = jax.checkpoint(group_forward)

    def one_group(item):
        return step_fn(lowered, norms, item[0], item[1])
    result = lax.map(one_group, (grouped, lengths))
    return result.reshape(TOKENS, D)

def adamw(master, first_moment, second_moment, average, gradient, step_rate, weight_decay):
    first_new = beta_one * first_moment + (1.0 - beta_one) * gradient
    second_new = beta_two * second_moment + (1.0 - beta_two) * gradient * gradient
    ratio = first_new / (1.0 - beta_one ** STEP) / (jnp.sqrt(second_new / (1.0 - beta_two ** STEP)) + epsilon)
    master_new = master - step_rate * (ratio + weight_decay * master)
    average_new = average_rate * average + (1.0 - average_rate) * master_new
    return (master_new, first_new, second_new, master_new.astype(jnp.bfloat16), average_new)

def reference(tokens, cotangent, lengths, qkv_master, qkv_first, qkv_second, qkv_average, out_master, out_first, out_second, out_average, up_master, up_first, up_second, up_average, down_master, down_first, down_second, down_average, norm_master, norm_first, norm_second, norm_average):

    def wrapped(rows_in, w_qkv, w_out, w_up, w_down, norms):
        return forward(rows_in, w_qkv, w_out, w_up, w_down, norms, lengths)
    layer_out, pullback = jax.vjp(wrapped, tokens, qkv_master, out_master, up_master, down_master, norm_master)
    input_grad, qkv_grad, out_grad, up_grad, down_grad, norm_grad = pullback(cotangent)
    qkv_new = adamw(qkv_master, qkv_first, qkv_second, qkv_average, qkv_grad, 0.02, 0.1)
    out_new = adamw(out_master, out_first, out_second, out_average, out_grad, 0.15, 0.1)
    up_new = adamw(up_master, up_first, up_second, up_average, up_grad, 0.02, 0.1)
    down_new = adamw(down_master, down_first, down_second, down_average, down_grad, 0.01, 0.1)
    norm_new = adamw(norm_master, norm_first, norm_second, norm_average, norm_grad, 0.5, 0.0)
    return (layer_out, input_grad, qkv_new[0], qkv_new[1], qkv_new[2], qkv_new[3], qkv_new[4], out_new[0], out_new[1], out_new[2], out_new[3], out_new[4], up_new[0], up_new[1], up_new[2], up_new[3], up_new[4], down_new[0], down_new[1], down_new[2], down_new[3], down_new[4], norm_new[0], norm_new[1], norm_new[2], norm_new[3], norm_new[4])
```

```python
import math

import jax
import jax.numpy as jnp
from jax import lax
from jax.sharding import PartitionSpec as P

HS = 256
ROT = 64
STEP = 7


beta_one = 0.9
beta_two = 0.95
epsilon = 1e-08
average_rate = 0.9


def rotary_tables(position):
    half_rot = ROT // 2
    exponent = jnp.arange(half_rot, dtype=jnp.float32) * (2.0 / ROT)
    inverse = jnp.exp(-math.log(10000.0) * exponent)
    angles = position[..., None] * inverse
    return (jnp.cos(angles), jnp.sin(angles))


def rotate(vectors, cosine, sine_table):
    half_rot = ROT // 2
    first_part = vectors[..., :half_rot]
    second_part = vectors[..., half_rot:ROT]
    return jnp.concatenate(
        [
            first_part * cosine - second_part * sine_table,
            second_part * cosine + first_part * sine_table,
            vectors[..., ROT:],
        ],
        axis=-1,
    )


def times(left, right):
    return jnp.dot(left, right, preferred_element_type=jnp.float32)


def times_transposed(left, right):
    return lax.dot_general(
        left, right, (((1,), (1,)), ((), ())), preferred_element_type=jnp.float32
    )


def transposed_times(left, right):
    return lax.dot_general(
        left, right, (((0,), (0,)), ((), ())), preferred_element_type=jnp.float32
    )


def swap_dp(value, bit):
    return lax.ppermute(value, "dp", [(d, d ^ bit) for d in range(lax.axis_size("dp"))])


def swap_tensor(value):
    return lax.ppermute(value, "tensor", [(0, 1), (1, 0)])


def plane_peers(own):
    return swap_tensor(own), swap_dp(own, 2)


def plane_blocks(own, along_t, along_x):
    half = own.shape[1] // 2
    diagonal = jnp.concatenate(
        [swap_dp(along_t[:, :half], 2), swap_tensor(along_x[:, half:])], axis=1
    )
    near = [own, along_t, along_x, diagonal]
    return near + [swap_dp(block, 1) for block in near]


def plane_sum(partial, rows):
    half = partial.shape[1] // 2
    low = jnp.bfloat16
    near = partial[: 4 * rows] + swap_dp(partial[4 * rows :], 1)
    own, along_t, along_x, diagonal = [near[i * rows : (i + 1) * rows] for i in range(4)]
    by_x = swap_dp(diagonal[:, :half].astype(low), 2).astype(jnp.float32)
    by_t = swap_tensor(diagonal[:, half:].astype(low)).astype(jnp.float32)
    along_t = jnp.concatenate([along_t[:, :half] + by_x, along_t[:, half:]], axis=1)
    along_x = jnp.concatenate([along_x[:, :half], along_x[:, half:] + by_t], axis=1)
    from_t = swap_tensor(along_t.astype(low)).astype(jnp.float32)
    from_x = swap_dp(along_x.astype(low), 2).astype(jnp.float32)
    return own + from_t + from_x


def total_sum(value):
    value = value + swap_tensor(value)
    bit = 1
    while bit < lax.axis_size("dp"):
        value = value + swap_dp(value, bit)
        bit *= 2
    return value


def regroup(shard, inner, inner_groups):
    rows, columns = shard.shape
    parts = shard.reshape(rows, inner, columns // inner).transpose(1, 0, 2)
    mine = lax.all_to_all(parts, "dp", 0, 0, axis_index_groups=inner_groups)
    return mine.reshape(inner * rows, columns // inner)


def outer_sum(grad, inner, outer_groups):
    n_outer = len(outer_groups[0])
    if n_outer != 4:
        return lax.psum_scatter(
            grad, "dp", scatter_dimension=0, axis_index_groups=outer_groups, tiled=True
        )
    low = jnp.bfloat16
    place = lax.axis_index("dp") // inner
    blocks = grad.reshape(n_outer, grad.shape[0] // n_outer, grad.shape[1])

    def pick(k):
        return lax.dynamic_index_in_dim(blocks, place ^ k, 0, keepdims=False)

    def move(value, ways):
        pairs = [(group[a], group[b]) for group in outer_groups for a, b in ways]
        return lax.ppermute(value, "dp", pairs)

    far = pick(3).astype(low)
    relayed = move(far, [(0, 1), (3, 2)]).astype(jnp.float32)
    middle = move(far, [(1, 2), (2, 1)]).astype(jnp.float32)
    next_to = move(pick(1).astype(low), [(0, 1), (1, 0), (2, 3), (3, 2)]).astype(jnp.float32)
    two_off = move((pick(2) + relayed).astype(low), [(0, 2), (2, 0), (1, 3), (3, 1)])
    return pick(0) + next_to + middle + two_off.astype(jnp.float32)


def ungroup(mine, inner, inner_groups):
    rows, columns = mine.shape
    parts = lax.all_to_all(
        mine.reshape(inner, rows // inner, columns), "dp", 0, 0, axis_index_groups=inner_groups
    )
    return parts.transpose(1, 0, 2)


def adamw(master, first_moment, second_moment, average, gradient, step_rate, weight_decay):
    first_new = beta_one * first_moment + (1.0 - beta_one) * gradient
    second_new = beta_two * second_moment + (1.0 - beta_two) * gradient * gradient
    ratio = (
        first_new
        / (1.0 - beta_one**STEP)
        / (jnp.sqrt(second_new / (1.0 - beta_two**STEP)) + epsilon)
    )
    master_new = master - step_rate * (ratio + weight_decay * master)
    average_new = average_rate * average + (1.0 - average_rate) * master_new
    return (master_new, first_new, second_new, master_new.astype(jnp.bfloat16), average_new)


def per_device(
    tokens,
    cotangent,
    lengths,
    qkv_master,
    qkv_first,
    qkv_second,
    qkv_average,
    out_master,
    out_first,
    out_second,
    out_average,
    up_master,
    up_first,
    up_second,
    up_average,
    down_master,
    down_first,
    down_second,
    down_average,
    norm_master,
    norm_first,
    norm_second,
    norm_average,
):
    low = jnp.bfloat16
    rows = tokens.shape[0]
    width = tokens.shape[1]
    inner = qkv_master.shape[1] // (3 * HS)
    n_dp = lax.axis_size("dp")
    n_outer = n_dp // inner
    inner_groups = [[o * inner + i for i in range(inner)] for o in range(n_outer)]
    outer_groups = [[o * inner + i for o in range(n_outer)] for i in range(inner)]
    scale = HS ** (-0.5)
    heads_dim = out_master.shape[0] // inner
    ff = down_master.shape[0] // inner

    shard_rows = qkv_master.shape[0]
    up_shard = up_master.astype(low)
    qkv_shard = qkv_master.astype(low)
    both_shard = jnp.concatenate(
        [
            down_master.astype(low).T.reshape(shard_rows, inner, ff),
            out_master.astype(low).T.reshape(shard_rows, inner, heads_dim),
        ],
        axis=2,
    ).reshape(shard_rows, inner * (ff + heads_dim))

    def gather(mine):
        return lax.all_gather(mine, "dp", axis=0, axis_index_groups=outer_groups, tiled=True)

    qkv_mine = regroup(qkv_shard, inner, inner_groups)
    tokens_t, tokens_x = plane_peers(tokens)
    w_qkv = gather(qkv_mine)
    tokens_t, tokens_x, up_shard = lax.optimization_barrier((tokens_t, tokens_x, up_shard))
    token_blocks = plane_blocks(tokens, tokens_t, tokens_x)
    w_up = gather(regroup(up_shard, inner, inner_groups))
    back_own, both_shard, token_blocks[3] = lax.optimization_barrier(
        (cotangent.astype(low), both_shard, token_blocks[3])
    )
    w_both = gather(regroup(both_shard, inner, inner_groups))
    back_blocks = plane_blocks(back_own, *plane_peers(back_own))
    rows_all = jnp.concatenate(token_blocks, axis=0)
    back = jnp.concatenate(back_blocks, axis=0)
    near_lengths = jnp.concatenate([lengths, swap_dp(lengths, 2)], axis=0)
    all_lengths = jnp.concatenate([near_lengths, swap_dp(near_lengths, 1)], axis=0)
    seqs = lengths.shape[1] // 2
    mine_first = lax.axis_index("tensor") == 0
    first_pair = all_lengths[:, 0]
    second_pair = all_lengths[:, seqs]
    own_first = jnp.where(mine_first, first_pair, second_pair)
    peer_first = jnp.where(mine_first, second_pair, first_pair)
    cut = jnp.stack([own_first, peer_first], axis=1).reshape(-1)

    average = jnp.mean(rows_all, axis=-1, keepdims=True)
    centered = rows_all - average
    variance = jnp.mean(centered * centered, axis=-1, keepdims=True)
    inverse_dev = lax.rsqrt(variance + 1e-05)
    hat = centered * inverse_dev
    rows_one = (hat * norm_master[0] + norm_master[1]).astype(low)
    rows_two = (hat * norm_master[2] + norm_master[3]).astype(low)

    upward = times(rows_two, w_up)
    gelu_value, gelu_pull = jax.vjp(lambda upper: jax.nn.gelu(upper, approximate=False), upward)
    active = gelu_value.astype(low)

    blocks = rows_all.shape[0] // rows
    row_index = jnp.arange(rows, dtype=jnp.int32)
    second = row_index[None, :] >= cut[:, None]
    position = (row_index[None, :] - jnp.where(second, cut[:, None], 0)).astype(jnp.float32)
    allowed = (second[:, :, None] == second[:, None, :]) & (
        row_index[:, None] >= row_index[None, :]
    )[None]
    cosine, sine_table = rotary_tables(position)
    joined = times(rows_one, w_qkv).reshape(blocks, rows, 3 * HS)
    query = rotate(joined[..., :HS], cosine, sine_table).astype(low)
    key = rotate(joined[..., HS : 2 * HS], cosine, sine_table).astype(low)
    value = joined[..., 2 * HS :].astype(low)
    scores = jnp.einsum("bqd,bkd->bqk", query, key, preferred_element_type=jnp.float32) * scale
    scores = jnp.where(allowed, scores, -1e30)
    probs = jax.nn.softmax(scores, axis=-1)
    probs_low = probs.astype(low)
    mixed = (
        jnp.einsum("bqk,bkd->bqd", probs_low, value, preferred_element_type=jnp.float32)
        .astype(low)
        .reshape(blocks * rows, HS)
    )

    inputs = jnp.concatenate([active, mixed], axis=1)
    both_grad = transposed_times(back, inputs)
    layer_out = tokens + plane_sum(times_transposed(inputs, w_both), rows)
    d_inputs = times(back, w_both)
    d_upward = gelu_pull(d_inputs[:, :ff])[0].astype(low)
    up_grad = transposed_times(rows_two, d_upward)
    d_mixed = d_inputs[:, ff:].astype(low).reshape(blocks, rows, HS)
    d_probs = jnp.einsum("bqd,bkd->bqk", d_mixed, value, preferred_element_type=jnp.float32)
    d_scores = (probs * (d_probs - jnp.sum(probs * d_probs, axis=-1, keepdims=True))).astype(low)
    d_value = jnp.einsum("bqk,bqd->bkd", probs_low, d_mixed, preferred_element_type=jnp.float32)
    d_query = jnp.einsum("bqk,bkd->bqd", d_scores, key, preferred_element_type=jnp.float32) * scale
    d_key = jnp.einsum("bqk,bqd->bkd", d_scores, query, preferred_element_type=jnp.float32) * scale
    d_joined = (
        jnp.concatenate(
            [rotate(d_query, cosine, -sine_table), rotate(d_key, cosine, -sine_table), d_value],
            axis=-1,
        )
        .astype(low)
        .reshape(blocks * rows, 3 * HS)
    )
    qkv_grad = transposed_times(rows_one, d_joined)

    both_sum = ungroup(outer_sum(both_grad, inner, outer_groups), inner, inner_groups)
    up_sum = ungroup(outer_sum(up_grad, inner, outer_groups), inner, inner_groups)
    qkv_sum = ungroup(outer_sum(qkv_grad, inner, outer_groups), inner, inner_groups)

    d_two = times_transposed(d_upward, w_up)
    d_one = times_transposed(d_joined, w_qkv)
    norm_local = jnp.stack(
        [
            jnp.sum(d_one * hat, axis=0),
            jnp.sum(d_one, axis=0),
            jnp.sum(d_two * hat, axis=0),
            jnp.sum(d_two, axis=0),
        ]
    )
    norm_grad = total_sum(norm_local)
    d_hat = plane_sum(d_one * norm_master[0] + d_two * norm_master[2], rows)
    own_hat = hat[:rows]
    input_grad = cotangent + inverse_dev[:rows] * (
        d_hat
        - jnp.mean(d_hat, axis=-1, keepdims=True)
        - own_hat * jnp.mean(d_hat * own_hat, axis=-1, keepdims=True)
    )

    down_sum = both_sum[..., :ff].reshape(shard_rows, inner * ff).T
    out_sum = both_sum[..., ff:].reshape(shard_rows, inner * heads_dim).T
    up_sum = up_sum.reshape(shard_rows, inner * ff)
    qkv_sum = qkv_sum.reshape(shard_rows, inner * 3 * HS)
    qkv_new = adamw(qkv_master, qkv_first, qkv_second, qkv_average, qkv_sum, 0.02, 0.1)
    out_new = adamw(out_master, out_first, out_second, out_average, out_sum, 0.15, 0.1)
    up_new = adamw(up_master, up_first, up_second, up_average, up_sum, 0.02, 0.1)
    down_new = adamw(down_master, down_first, down_second, down_average, down_sum, 0.01, 0.1)
    norm_new = adamw(norm_master, norm_first, norm_second, norm_average, norm_grad, 0.5, 0.0)
    return (
        layer_out,
        input_grad,
        qkv_new[0],
        qkv_new[1],
        qkv_new[2],
        qkv_new[3],
        qkv_new[4],
        out_new[0],
        out_new[1],
        out_new[2],
        out_new[3],
        out_new[4],
        up_new[0],
        up_new[1],
        up_new[2],
        up_new[3],
        up_new[4],
        down_new[0],
        down_new[1],
        down_new[2],
        down_new[3],
        down_new[4],
        norm_new[0],
        norm_new[1],
        norm_new[2],
        norm_new[3],
        norm_new[4],
    )


def solution(mesh):
    placed = (
        P(("dp", "tensor"), None),
        P(("dp", "tensor"), None),
        P("dp", None),
        P("dp", "tensor"),
        P("dp", "tensor"),
        P("dp", "tensor"),
        P("dp", "tensor"),
        P("tensor", "dp"),
        P("tensor", "dp"),
        P("tensor", "dp"),
        P("tensor", "dp"),
        P("dp", "tensor"),
        P("dp", "tensor"),
        P("dp", "tensor"),
        P("dp", "tensor"),
        P("tensor", "dp"),
        P("tensor", "dp"),
        P("tensor", "dp"),
        P("tensor", "dp"),
        P(),
        P(),
        P(),
        P(),
    )
    return jax.shard_map(
        per_device,
        mesh=mesh,
        in_specs=placed,
        out_specs=(
            P(("dp", "tensor"), None),
            P(("dp", "tensor"), None),
            P("dp", "tensor"),
            P("dp", "tensor"),
            P("dp", "tensor"),
            P("dp", "tensor"),
            P("dp", "tensor"),
            P("tensor", "dp"),
            P("tensor", "dp"),
            P("tensor", "dp"),
            P("tensor", "dp"),
            P("tensor", "dp"),
            P("dp", "tensor"),
            P("dp", "tensor"),
            P("dp", "tensor"),
            P("dp", "tensor"),
            P("dp", "tensor"),
            P("tensor", "dp"),
            P("tensor", "dp"),
            P("tensor", "dp"),
            P("tensor", "dp"),
            P("tensor", "dp"),
            P(),
            P(),
            P(),
            P(),
            P(),
        ),
        check_vma=False,
    )
```
